32 devices in a mesh: gy: 8 (over y, x, core), gx: 4 (over z).
Axes of the slice: x: 2, y: 2, z: 4, core: 2. Of those that a mesh axis runs over, the one named last changes fastest.
Arguments:
- left_factor: bfloat16 [8192, 2048], P('gy', 'gx'), may hold values from -6 to 6
- right_factor: bfloat16 [2048, 8192], P('gy', 'gx'), may hold values from -0.125 to 0.125
Outputs:
- corrected: float32 [8192, 8192], P('gy', 'gx')
The draws below stay inside these ranges and needn't reach their ends.
All inputs are finite; a program needn't handle non-finite values.
Results may differ from the reference program's by a relative error of at most 0.0003.
Values may be sent and summed in bfloat16 or wider, within the bound.
A program may use at most 192 MiB of HBM per device.

```python
import jax
import jax.numpy as jnp
from jax import lax

ROWS = 8192
COLS = 8192
INNER = 2048


def shard_levels(key, shape, shards, smallest, high):
    loudness, own = 1.0, jax.random.fold_in(key, 6)
    for dim, blocks in shards:
        steps = jnp.exp(jax.random.uniform(jax.random.fold_in(own, dim), (blocks,), jnp.float32, smallest / len(shards), high / len(shards)))
        loudness = loudness * jnp.repeat(steps, shape[dim] // blocks).reshape([-1 if axis == dim else 1 for axis in range(len(shape))])
    return loudness


def scatter_about(own_key, shape, spread, most, split=(), kind=jnp.bfloat16):
    drawn = spread * jax.random.normal(own_key, shape, jnp.float32)
    if split:
        drawn = drawn * shard_levels(own_key, shape, split, -0.22, 0.18)
    return jnp.clip(drawn, -most, most).astype(kind)


def setup_inputs(seed: int = 0) -> dict:
    splits = jax.random.split(jax.random.key(seed), 3)
    return {
        "left_factor": scatter_about(splits[0], (ROWS, INNER), 1.0, 6.0, ((0, 8), (1, 4))),
        "right_factor": scatter_about(splits[1], (INNER, COLS), INNER ** -0.5, 0.125, ((0, 8), (1, 4))),
    }


def reference(left_factor, right_factor):
    corrected = jnp.dot(left_factor, right_factor, preferred_element_type=jnp.float32)
    row_power = lax.optimization_barrier(jnp.sum(corrected * corrected, axis=1))
    corrected = corrected * lax.rsqrt(row_power / COLS + 1e-06)[:, None]
    return corrected
```

```python
import functools

import jax
import jax.numpy as jnp
from jax import lax
from jax.experimental import pallas as pl
from jax.experimental.pallas import tpu as pltpu
from jax.sharding import PartitionSpec as P

MESH = pl.DeviceIdType.MESH
CHUNK = 128
CORES = 2


def other_chip(chip, offset, chips):
    if chips & (chips - 1):
        return (chip + offset) % chips
    for bit in range(chips.bit_length() - 1):
        if (offset >> bit) & 1:
            chip = chip + (1 << bit) * (1 - 2 * ((chip // (1 << bit)) % 2))
    return chip


def kernel(m, n, left, right, acc, scale, a, b, power, own_sem, a_send, a_recv, b_send, b_pass, b_recv, p_send, p_recv):
    gy, gx = lax.axis_index("gy"), lax.axis_index("gx")
    rows, ka = left.shape
    kb, cols = right.shape
    chunks, chips = rows // CHUNK, m // CORES
    chip, core = gy // CORES, gy % CORES
    partner = chip * CORES + (1 - core)
    has_right, has_left = gx < n - 1, gx > 0

    def peer(offset, which):
        return other_chip(chip, offset, chips) * CORES + which

    barrier = pltpu.get_barrier_semaphore()
    greeted = [(peer(p, core), gx) for p in range(1, chips)] + [(partner, gx)]
    greeted += [(gy, (gx + d) % n) for d in range(1, n)]
    for device in greeted:
        pl.semaphore_signal(barrier, inc=1, device_id=device, device_id_type=MESH)
    pl.semaphore_wait(barrier, len(greeted))

    def a_slot(block, r):
        return a.at[
            pl.ds(pl.multiple_of(r * CHUNK, CHUNK), CHUNK),
            pl.ds(pl.multiple_of(block * ka, ka), ka),
        ]

    def a_copy(block, r, way, source=None):
        return pltpu.make_async_remote_copy(
            src_ref=a_slot(block, r) if source is None else source,
            dst_ref=a_slot(block, r),
            send_sem=a_send.at[way, block, r],
            recv_sem=a_recv.at[block, r],
            device_id=(gy, gx + 2 * way - 1),
            device_id_type=MESH,
        )

    def own_a(r, way):
        return a_copy(gx, r, way, left.at[pl.ds(pl.multiple_of(r * CHUNK, CHUNK), CHUNK), :])

    def b_slot(block):
        return b.at[pl.ds(pl.multiple_of(block * kb, kb), kb), :]

    def b_copy(p):
        return pltpu.make_async_remote_copy(
            src_ref=right,
            dst_ref=b_slot(gy),
            send_sem=b_send.at[p],
            recv_sem=b_recv.at[gy],
            device_id=(partner, gx) if p == 0 else (peer(p, core), gx),
            device_id_type=MESH,
        )

    def b_onward(p):
        block = peer(p, core)
        return pltpu.make_async_remote_copy(
            src_ref=b_slot(block),
            dst_ref=b_slot(block),
            send_sem=b_pass.at[p],
            recv_sem=b_recv.at[block],
            device_id=(partner, gx),
            device_id_type=MESH,
        )

    def b_arrival(block):
        return pltpu.make_async_remote_copy(
            src_ref=b_slot(block),
            dst_ref=b_slot(block),
            send_sem=b_pass.at[0],
            recv_sem=b_recv.at[block],
            device_id=(partner, gx),
            device_id_type=MESH,
        )

    def each_chunk(body):
        lax.fori_loop(0, chunks, lambda r, carry: (body(r), carry)[1], 0)

    @each_chunk
    def _(r):
        @pl.when(has_right)
        def _():
            own_a(r, 1).start()

        @pl.when(has_left)
        def _():
            own_a(r, 0).start()

    for p in [*range(1, chips), 0]:
        b_copy(p).start()
    keep_a = pltpu.make_async_copy(left, a.at[:, pl.ds(pl.multiple_of(gx * ka, ka), ka)], own_sem.at[0])
    keep_b = pltpu.make_async_copy(right, b_slot(gy), own_sem.at[1])
    keep_a.start()
    keep_b.start()

    def pass_b(p):
        b_arrival(peer(p, core)).wait_recv()
        b_onward(p).start()

    def relay(d, r, act):
        @pl.when(jnp.logical_and(gx >= d, has_right))
        def _():
            act(gx - d, r, 1)

        @pl.when(jnp.logical_and(gx + d < n, has_left))
        def _():
            act(gx + d, r, 0)

    def receive_and_pass(block, r, way):
        a_copy(block, r, way).wait_recv()
        a_copy(block, r, way).start()

    early = max(chips - 2, 0)
    for d in range(1, n - 1):
        each_chunk(lambda r: relay(d, r, receive_and_pass))
        if d == 1:
            for p in range(1, 1 + early):
                pass_b(p)
    for p in range(1 + (early if n > 2 else 0), chips):
        pass_b(p)

    keep_a.wait()
    keep_b.wait()
    at_end = jnp.logical_or(gx == 0, gx == n - 1)
    for block in range(1, n - 1):

        @each_chunk
        def _(r):
            @pl.when(at_end)
            def _():
                a_copy(block, r, 0).wait_recv()

    for p in range(chips):
        b_arrival(peer(p, 1 - core)).wait_recv()

    upper = (2 * gx) // n
    far = (n - 1) * (1 - upper)
    near_k = (n - 1) * ka
    near = pl.ds(pl.multiple_of(upper * ka, ka), near_k)
    far_k = pl.ds(pl.multiple_of(far * ka, ka), ka)
    wide = 512 if cols % 512 == 0 else cols
    tall = 256 if rows % 256 == 0 else CHUNK

    def near_tile(i, carry):
        tile_rows = pl.ds(pl.multiple_of((i // (cols // wide)) * tall, tall), tall)
        tile_cols = pl.ds(pl.multiple_of((i % (cols // wide)) * wide, wide), wide)
        acc[tile_rows, tile_cols] = jnp.dot(
            a[tile_rows, near], b[near, tile_cols], preferred_element_type=jnp.float32
        )
        return carry

    lax.fori_loop(0, (rows // tall) * (cols // wide), near_tile, 0)

    @each_chunk
    def _(r):
        @pl.when(at_end)
        def _():
            a_copy(far, r, 0).wait_recv()

        here = pl.ds(pl.multiple_of(r * CHUNK, CHUNK), CHUNK)
        squares = jnp.zeros((CHUNK, 128), jnp.float32)
        for c in range(0, cols, wide):
            tile = acc[here, c : c + wide] + jnp.dot(
                a[here, far_k], b[far_k, c : c + wide], preferred_element_type=jnp.float32
            )
            acc[here, c : c + wide] = tile
            for lane in range(0, wide, 128):
                squares = squares + tile[:, lane : lane + 128] * tile[:, lane : lane + 128]
        power[gx, pl.ds(r, 1), :] = jnp.sum(squares.T, axis=0, keepdims=True)

    def p_copy(d, block):
        return pltpu.make_async_remote_copy(
            src_ref=power.at[block],
            dst_ref=power.at[block],
            send_sem=p_send.at[d],
            recv_sem=p_recv.at[block],
            device_id=(gy, (gx + d) % n),
            device_id_type=MESH,
        )

    for d in range(1, n):
        p_copy(d, gx).start()

    @each_chunk
    def _(r):
        @pl.when(has_right)
        def _():
            own_a(r, 1).wait_send()

        @pl.when(has_left)
        def _():
            own_a(r, 0).wait_send()

        for d in range(1, n - 1):
            relay(d, r, lambda block, r, way: a_copy(block, r, way).wait_send())

    for p in range(chips):
        b_copy(p).wait_send()
        if p:
            b_onward(p).wait_send()
    for d in range(1, n):
        p_copy(d, (gx + d) % n).wait_recv()
    total = power[0]
    for z in range(1, n):
        total = total + power[z]
    scale[...] = lax.rsqrt(total / (cols * n) + 1e-06)
    for d in range(1, n):
        p_copy(d, gx).wait_send()


def per_device(m, n, left_factor, right_factor):
    rows, ka = left_factor.shape
    kb, cols = right_factor.shape
    chunks, chips = rows // CHUNK, m // CORES
    dma = pltpu.SemaphoreType.DMA
    product, scale = pl.pallas_call(
        functools.partial(kernel, m, n),
        out_shape=[
            pltpu.VMEM((rows, cols), jnp.float32),
            jax.ShapeDtypeStruct((chunks, 128), jnp.float32),
        ],
        in_specs=[pl.BlockSpec(memory_space=pl.ANY)] * 2,
        out_specs=[pl.BlockSpec(memory_space=pltpu.VMEM)] * 2,
        scratch_shapes=[
            pltpu.VMEM((rows, n * ka), left_factor.dtype),
            pltpu.VMEM((m * kb, cols), right_factor.dtype),
            pltpu.VMEM((n, chunks, 128), jnp.float32),
            dma((2,)),
            dma((2, n, chunks)),
            dma((n, chunks)),
            dma((chips,)),
            dma((chips,)),
            dma((m,)),
            dma((n,)),
            dma((n,)),
        ],
        compiler_params=pltpu.CompilerParams(
            collective_id=0,
            has_side_effects=True,
            vmem_limit_bytes=n * ka * rows * 2 + m * kb * cols * 2 + 5 * 2**20,
        ),
    )(left_factor, right_factor)
    return product * scale.reshape(rows)[:, None]


def solution(mesh):
    placed = (P("gy", "gx"), P("gy", "gx"))
    return jax.shard_map(
        functools.partial(per_device, mesh.shape["gy"], mesh.shape["gx"]),
        mesh=mesh,
        in_specs=placed,
        out_specs=P("gy", "gx"),
        check_vma=False,
    )
```

```python
import functools

import jax
import jax.numpy as jnp
from jax import lax
from jax.experimental import pallas as pl
from jax.experimental.pallas import tpu as pltpu
from jax.sharding import PartitionSpec as P

MESH = pl.DeviceIdType.MESH
CHUNK = 128
CORES = 2
VMEM_BYTES = 67043328


def other_chip(chip, offset, chips):
    if chips & (chips - 1):
        return (chip + offset) % chips
    for bit in range(chips.bit_length() - 1):
        if (offset >> bit) & 1:
            chip = chip + (1 << bit) * (1 - 2 * ((chip // (1 << bit)) % 2))
    return chip


def kernel(m, n, left, right, acc, scale, a, b, power, own_sem, a_send, a_recv, b_send, b_pass, b_recv, p_send, p_recv):
    gy, gx = lax.axis_index("gy"), lax.axis_index("gx")
    rows, ka = left.shape
    kb, cols = right.shape
    chunks, chips = rows // CHUNK, m // CORES
    chip, core = gy // CORES, gy % CORES
    partner = chip * CORES + (1 - core)
    has_right, has_left = gx < n - 1, gx > 0

    def peer(offset, which):
        return other_chip(chip, offset, chips) * CORES + which

    barrier = pltpu.get_barrier_semaphore()
    greeted = [(peer(p, core), gx) for p in range(1, chips)] + [(partner, gx)]
    greeted += [(gy, (gx + d) % n) for d in range(1, n)]
    for device in greeted:
        pl.semaphore_signal(barrier, inc=1, device_id=device, device_id_type=MESH)
    pl.semaphore_wait(barrier, len(greeted))

    def a_slot(block, r):
        return a.at[
            pl.ds(pl.multiple_of(r * CHUNK, CHUNK), CHUNK),
            pl.ds(pl.multiple_of(block * ka, ka), ka),
        ]

    def a_copy(block, r, way, source=None):
        return pltpu.make_async_remote_copy(
            src_ref=a_slot(block, r) if source is None else source,
            dst_ref=a_slot(block, r),
            send_sem=a_send.at[way, block, r],
            recv_sem=a_recv.at[block, r],
            device_id=(gy, gx + 2 * way - 1),
            device_id_type=MESH,
        )

    def own_a(r, way):
        return a_copy(gx, r, way, left.at[pl.ds(pl.multiple_of(r * CHUNK, CHUNK), CHUNK), :])

    def b_slot(block):
        return b.at[pl.ds(pl.multiple_of(block * kb, kb), kb), :]

    def b_copy(p):
        return pltpu.make_async_remote_copy(
            src_ref=right,
            dst_ref=b_slot(gy),
            send_sem=b_send.at[p],
            recv_sem=b_recv.at[gy],
            device_id=(partner, gx) if p == 0 else (peer(p, core), gx),
            device_id_type=MESH,
        )

    def b_onward(p):
        block = peer(p, core)
        return pltpu.make_async_remote_copy(
            src_ref=b_slot(block),
            dst_ref=b_slot(block),
            send_sem=b_pass.at[p],
            recv_sem=b_recv.at[block],
            device_id=(partner, gx),
            device_id_type=MESH,
        )

    def b_arrival(block):
        return pltpu.make_async_remote_copy(
            src_ref=b_slot(block),
            dst_ref=b_slot(block),
            send_sem=b_pass.at[0],
            recv_sem=b_recv.at[block],
            device_id=(partner, gx),
            device_id_type=MESH,
        )

    def each_chunk(body):
        lax.fori_loop(0, chunks, lambda r, carry: (body(r), carry)[1], 0)

    @each_chunk
    def _(r):
        @pl.when(has_right)
        def _():
            own_a(r, 1).start()

        @pl.when(has_left)
        def _():
            own_a(r, 0).start()

    for p in [*range(1, chips), 0]:
        b_copy(p).start()
    keep_a = pltpu.make_async_copy(left, a.at[:, pl.ds(pl.multiple_of(gx * ka, ka), ka)], own_sem.at[0])
    keep_b = pltpu.make_async_copy(right, b_slot(gy), own_sem.at[1])
    keep_a.start()
    keep_b.start()

    def pass_b(p):
        b_arrival(peer(p, core)).wait_recv()
        b_onward(p).start()

    def relay(d, r, act):
        @pl.when(jnp.logical_and(gx >= d, has_right))
        def _():
            act(gx - d, r, 1)

        @pl.when(jnp.logical_and(gx + d < n, has_left))
        def _():
            act(gx + d, r, 0)

    def receive_and_pass(block, r, way):
        a_copy(block, r, way).wait_recv()
        a_copy(block, r, way).start()

    early = max(chips - 2, 0)
    for d in range(1, n - 1):
        each_chunk(lambda r: relay(d, r, receive_and_pass))
        if d == 1:
            for p in range(1, 1 + early):
                pass_b(p)
    for p in range(1 + (early if n > 2 else 0), chips):
        pass_b(p)

    keep_a.wait()
    keep_b.wait()
    at_end = jnp.logical_or(gx == 0, gx == n - 1)
    for block in range(1, n - 1):

        @each_chunk
        def _(r):
            @pl.when(at_end)
            def _():
                a_copy(block, r, 0).wait_recv()

    for p in range(chips):
        b_arrival(peer(p, 1 - core)).wait_recv()

    upper = (2 * gx) // n
    far = (n - 1) * (1 - upper)
    near_k = (n - 1) * ka
    near = pl.ds(pl.multiple_of(upper * ka, ka), near_k)
    far_k = pl.ds(pl.multiple_of(far * ka, ka), ka)
    wide = 512 if cols % 512 == 0 else cols
    tall = 256 if rows % 256 == 0 else CHUNK

    def near_tile(i, carry):
        tile_rows = pl.ds(pl.multiple_of((i // (cols // wide)) * tall, tall), tall)
        tile_cols = pl.ds(pl.multiple_of((i % (cols // wide)) * wide, wide), wide)
        acc[tile_rows, tile_cols] = jnp.dot(
            a[tile_rows, near], b[near, tile_cols], preferred_element_type=jnp.float32
        )
        return carry

    lax.fori_loop(0, (rows // tall) * (cols // wide), near_tile, 0)

    @each_chunk
    def _(r):
        @pl.when(at_end)
        def _():
            a_copy(far, r, 0).wait_recv()

        here = pl.ds(pl.multiple_of(r * CHUNK, CHUNK), CHUNK)
        squares = jnp.zeros((CHUNK, 128), jnp.float32)
        for c in range(0, cols, wide):
            tile = acc[here, c : c + wide] + jnp.dot(
                a[here, far_k], b[far_k, c : c + wide], preferred_element_type=jnp.float32
            )
            acc[here, c : c + wide] = tile
            for lane in range(0, wide, 128):
                squares = squares + tile[:, lane : lane + 128] * tile[:, lane : lane + 128]
        power[gx, pl.ds(r, 1), :] = jnp.sum(squares.T, axis=0, keepdims=True)

    def p_copy(d, block):
        return pltpu.make_async_remote_copy(
            src_ref=power.at[block],
            dst_ref=power.at[block],
            send_sem=p_send.at[d],
            recv_sem=p_recv.at[block],
            device_id=(gy, (gx + d) % n),
            device_id_type=MESH,
        )

    for d in range(1, n):
        p_copy(d, gx).start()

    @each_chunk
    def _(r):
        @pl.when(has_right)
        def _():
            own_a(r, 1).wait_send()

        @pl.when(has_left)
        def _():
            own_a(r, 0).wait_send()

        for d in range(1, n - 1):
            relay(d, r, lambda block, r, way: a_copy(block, r, way).wait_send())

    for p in range(chips):
        b_copy(p).wait_send()
        if p:
            b_onward(p).wait_send()
    for d in range(1, n):
        p_copy(d, (gx + d) % n).wait_recv()
    total = power[0]
    for z in range(1, n):
        total = total + power[z]
    scale[...] = lax.rsqrt(total / (cols * n) + 1e-06)
    for d in range(1, n):
        p_copy(d, gx).wait_send()


def finish(product, scale, out, staged, sem):
    rows, cols = product.shape

    def copy(r):
        here = pl.ds(pl.multiple_of(r * CHUNK, CHUNK), CHUNK)
        return pltpu.make_async_copy(staged.at[here], out.at[here], sem.at[r])

    def scale_chunk(r, carry):
        here = pl.ds(pl.multiple_of(r * CHUNK, CHUNK), CHUNK)
        by_row = jnp.broadcast_to(scale[pl.ds(r, 1), :], (CHUNK, CHUNK)).T
        for lane in range(0, cols, CHUNK):
            staged[here, lane : lane + CHUNK] = product[here, lane : lane + CHUNK] * by_row
        copy(r).start()
        return carry

    lax.fori_loop(0, rows // CHUNK, scale_chunk, 0)
    for r in range(rows // CHUNK):
        copy(r).wait()


def per_device(m, n, left_factor, right_factor):
    rows, ka = left_factor.shape
    kb, cols = right_factor.shape
    chunks, chips = rows // CHUNK, m // CORES
    dma = pltpu.SemaphoreType.DMA
    product, scale = pl.pallas_call(
        functools.partial(kernel, m, n),
        out_shape=[
            pltpu.VMEM((rows, cols), jnp.float32),
            pltpu.VMEM((chunks, 128), jnp.float32),
        ],
        in_specs=[pl.BlockSpec(memory_space=pltpu.HBM)] * 2,
        out_specs=[pl.BlockSpec(memory_space=pltpu.VMEM)] * 2,
        scratch_shapes=[
            pltpu.VMEM((rows, n * ka), left_factor.dtype),
            pltpu.VMEM((m * kb, cols), right_factor.dtype),
            pltpu.VMEM((n, chunks, 128), jnp.float32),
            dma((2,)),
            dma((2, n, chunks)),
            dma((n, chunks)),
            dma((chips,)),
            dma((chips,)),
            dma((m,)),
            dma((n,)),
            dma((n,)),
        ],
        compiler_params=pltpu.CompilerParams(
            collective_id=0,
            has_side_effects=True,
            vmem_limit_bytes=VMEM_BYTES - rows * cols * 4 - 2**19,
        ),
    )(left_factor, right_factor)
    return pl.pallas_call(
        finish,
        out_shape=jax.ShapeDtypeStruct((rows, cols), jnp.float32),
        in_specs=[pl.BlockSpec(memory_space=pltpu.VMEM)] * 2,
        out_specs=pl.BlockSpec(memory_space=pl.ANY),
        scratch_shapes=[pltpu.VMEM((rows, cols), jnp.float32), dma((chunks,))],
        compiler_params=pltpu.CompilerParams(vmem_limit_bytes=rows * cols * 4 + 2 * 2**20),
    )(product, scale)


def solution(mesh):
    placed = (P("gy", "gx"), P("gy", "gx"))
    return jax.shard_map(
        functools.partial(per_device, mesh.shape["gy"], mesh.shape["gx"]),
        mesh=mesh,
        in_specs=placed,
        out_specs=P("gy", "gx"),
        check_vma=False,
    )
```

```python
import functools

import jax
import jax.numpy as jnp
from jax import lax
from jax.experimental import pallas as pl
from jax.experimental.pallas import tpu as pltpu
from jax.sharding import PartitionSpec as P

MESH = pl.DeviceIdType.MESH
CHUNK = 128
CORES = 2
TAIL = 2
VMEM_BYTES = 67043328


def other_chip(chip, offset, chips):
    if chips & (chips - 1):
        return (chip + offset) % chips
    for bit in range(chips.bit_length() - 1):
        if (offset >> bit) & 1:
            chip = chip + (1 << bit) * (1 - 2 * ((chip // (1 << bit)) % 2))
    return chip


def kernel(m, n, left, right, acc, scale, a, b, power, tail_power, early_scale, own_sem, a_send, a_recv, b_send, b_pass, b_recv, p_send, p_recv):
    gy, gx = lax.axis_index("gy"), lax.axis_index("gx")
    rows, ka = left.shape
    kb, cols = right.shape
    chunks, chips = rows // CHUNK, m // CORES
    chip, core = gy // CORES, gy % CORES
    partner = chip * CORES + (1 - core)
    has_right, has_left = gx < n - 1, gx > 0

    def peer(offset, which):
        return other_chip(chip, offset, chips) * CORES + which

    barrier = pltpu.get_barrier_semaphore()
    greeted = [(peer(p, core), gx) for p in range(1, chips)] + [(partner, gx)]
    greeted += [(gy, (gx + d) % n) for d in range(1, n)]
    for device in greeted:
        pl.semaphore_signal(barrier, inc=1, device_id=device, device_id_type=MESH)
    pl.semaphore_wait(barrier, len(greeted))

    def a_slot(block, r):
        return a.at[
            pl.ds(pl.multiple_of(r * CHUNK, CHUNK), CHUNK),
            pl.ds(pl.multiple_of(block * ka, ka), ka),
        ]

    def a_copy(block, r, way, source=None):
        return pltpu.make_async_remote_copy(
            src_ref=a_slot(block, r) if source is None else source,
            dst_ref=a_slot(block, r),
            send_sem=a_send.at[way, block, r],
            recv_sem=a_recv.at[block, r],
            device_id=(gy, gx + 2 * way - 1),
            device_id_type=MESH,
        )

    def own_a(r, way):
        return a_copy(gx, r, way, left.at[pl.ds(pl.multiple_of(r * CHUNK, CHUNK), CHUNK), :])

    def b_slot(block):
        return b.at[pl.ds(pl.multiple_of(block * kb, kb), kb), :]

    def b_copy(p):
        return pltpu.make_async_remote_copy(
            src_ref=right,
            dst_ref=b_slot(gy),
            send_sem=b_send.at[p],
            recv_sem=b_recv.at[gy],
            device_id=(partner, gx) if p == 0 else (peer(p, core), gx),
            device_id_type=MESH,
        )

    def b_onward(p):
        block = peer(p, core)
        return pltpu.make_async_remote_copy(
            src_ref=b_slot(block),
            dst_ref=b_slot(block),
            send_sem=b_pass.at[p],
            recv_sem=b_recv.at[block],
            device_id=(partner, gx),
            device_id_type=MESH,
        )

    def b_arrival(block):
        return pltpu.make_async_remote_copy(
            src_ref=b_slot(block),
            dst_ref=b_slot(block),
            send_sem=b_pass.at[0],
            recv_sem=b_recv.at[block],
            device_id=(partner, gx),
            device_id_type=MESH,
        )

    def each_chunk(body):
        lax.fori_loop(0, chunks, lambda r, carry: (body(r), carry)[1], 0)

    @each_chunk
    def _(r):
        @pl.when(has_right)
        def _():
            own_a(r, 1).start()

        @pl.when(has_left)
        def _():
            own_a(r, 0).start()

    for p in [*range(1, chips), 0]:
        b_copy(p).start()
    keep_a = pltpu.make_async_copy(left, a.at[:, pl.ds(pl.multiple_of(gx * ka, ka), ka)], own_sem.at[0])
    keep_b = pltpu.make_async_copy(right, b_slot(gy), own_sem.at[1])
    keep_a.start()
    keep_b.start()

    def pass_b(p):
        b_arrival(peer(p, core)).wait_recv()
        b_onward(p).start()

    def relay(d, r, act):
        @pl.when(jnp.logical_and(gx >= d, has_right))
        def _():
            act(gx - d, r, 1)

        @pl.when(jnp.logical_and(gx + d < n, has_left))
        def _():
            act(gx + d, r, 0)

    def receive_and_pass(block, r, way):
        a_copy(block, r, way).wait_recv()
        a_copy(block, r, way).start()

    early = max(chips - 2, 0)
    for d in range(1, n - 1):
        each_chunk(lambda r: relay(d, r, receive_and_pass))
        if d == 1:
            for p in range(1, 1 + early):
                pass_b(p)
    for p in range(1 + (early if n > 2 else 0), chips):
        pass_b(p)

    keep_a.wait()
    keep_b.wait()
    at_end = jnp.logical_or(gx == 0, gx == n - 1)
    for block in range(1, n - 1):

        @each_chunk
        def _(r):
            @pl.when(at_end)
            def _():
                a_copy(block, r, 0).wait_recv()

    for p in range(chips):
        b_arrival(peer(p, 1 - core)).wait_recv()

    upper = (2 * gx) // n
    far = (n - 1) * (1 - upper)
    near_k = (n - 1) * ka
    near = pl.ds(pl.multiple_of(upper * ka, ka), near_k)
    far_k = pl.ds(pl.multiple_of(far * ka, ka), ka)
    wide = 512 if cols % 512 == 0 else cols
    tall = 256 if rows % 256 == 0 else CHUNK

    def near_tile(i, carry):
        tile_rows = pl.ds(pl.multiple_of((i // (cols // wide)) * tall, tall), tall)
        tile_cols = pl.ds(pl.multiple_of((i % (cols // wide)) * wide, wide), wide)
        acc[tile_rows, tile_cols] = jnp.dot(
            a[tile_rows, near], b[near, tile_cols], preferred_element_type=jnp.float32
        )
        return carry

    lax.fori_loop(0, (rows // tall) * (cols // wide), near_tile, 0)

    def far_chunk(r):
        @pl.when(at_end)
        def _():
            a_copy(far, r, 0).wait_recv()

        here = pl.ds(pl.multiple_of(r * CHUNK, CHUNK), CHUNK)
        squares = jnp.zeros((CHUNK, 128), jnp.float32)
        for c in range(0, cols, wide):
            tile = acc[here, c : c + wide] + jnp.dot(
                a[here, far_k], b[far_k, c : c + wide], preferred_element_type=jnp.float32
            )
            acc[here, c : c + wide] = tile
            for lane in range(0, wide, 128):
                squares = squares + tile[:, lane : lane + 128] * tile[:, lane : lane + 128]
        return jnp.sum(squares.T, axis=0, keepdims=True)

    def early_chunk(r, carry):
        power[gx, pl.ds(r, 1), :] = far_chunk(r)
        return carry

    def share(which, block, d):
        part = (power, tail_power)[which].at[block]
        return pltpu.make_async_remote_copy(
            src_ref=part,
            dst_ref=part,
            send_sem=p_send.at[which, d],
            recv_sem=p_recv.at[which, block],
            device_id=(gy, (gx + d) % n),
            device_id_type=MESH,
        )

    def gathered(which):
        sums = (power, tail_power)[which]
        for d in range(1, n):
            share(which, (gx + d) % n, d).wait_recv()
        total = sums[0]
        for z in range(1, n):
            total = total + sums[z]
        return lax.rsqrt(total / (cols * n) + 1e-06)

    first = chunks - TAIL
    power[gx] = jnp.zeros((chunks, 128), jnp.float32)
    tail_power[gx] = jnp.zeros((8, 128), jnp.float32)
    lax.fori_loop(0, first, early_chunk, 0)
    for d in range(1, n):
        share(0, gx, d).start()
    for r in range(TAIL):
        tail_power[gx, pl.ds(r, 1), :] = far_chunk(first + r)
    for d in range(1, n):
        share(1, gx, d).start()

    early_scale[...] = gathered(0)

    def scale_chunk(r, carry):
        here = pl.ds(pl.multiple_of(r * CHUNK, CHUNK), CHUNK)
        factor = by_row(early_scale[pl.ds(r, 1), :])
        for lane in range(0, cols, CHUNK):
            acc[here, lane : lane + CHUNK] = acc[here, lane : lane + CHUNK] * factor
        return carry

    lax.fori_loop(0, first, scale_chunk, 0)

    @each_chunk
    def _(r):
        @pl.when(has_right)
        def _():
            own_a(r, 1).wait_send()

        @pl.when(has_left)
        def _():
            own_a(r, 0).wait_send()

        for d in range(1, n - 1):
            relay(d, r, lambda block, r, way: a_copy(block, r, way).wait_send())

    for p in range(chips):
        b_copy(p).wait_send()
        if p:
            b_onward(p).wait_send()
    for d in range(1, n):
        share(0, gx, d).wait_send()
        share(1, gx, d).wait_send()
    scale[...] = gathered(1)


def by_row(sums):
    return jnp.broadcast_to(sums, (CHUNK, CHUNK)).T


def finish(product, scale, out, staged, sem):
    rows, cols = product.shape
    chunks = rows // CHUNK
    first = chunks - TAIL

    def copy(r):
        here = pl.ds(r * CHUNK, CHUNK)
        source = product.at[here] if r < first else staged.at[r - first]
        return pltpu.make_async_copy(source, out.at[here], sem.at[r])

    for r in range(first):
        copy(r).start()
    for r in range(first, chunks):
        factor = by_row(scale[r - first : r - first + 1, :])
        for lane in range(0, cols, CHUNK):
            staged[r - first, :, lane : lane + CHUNK] = (
                product[r * CHUNK : (r + 1) * CHUNK, lane : lane + CHUNK] * factor
            )
        copy(r).start()
    for r in range(chunks):
        copy(r).wait()


def per_device(m, n, left_factor, right_factor):
    rows, ka = left_factor.shape
    kb, cols = right_factor.shape
    chunks, chips = rows // CHUNK, m // CORES
    dma = pltpu.SemaphoreType.DMA
    product, scale = pl.pallas_call(
        functools.partial(kernel, m, n),
        out_shape=[
            pltpu.VMEM((rows, cols), jnp.float32),
            pltpu.VMEM((8, 128), jnp.float32),
        ],
        in_specs=[pl.BlockSpec(memory_space=pltpu.HBM)] * 2,
        out_specs=[pl.BlockSpec(memory_space=pltpu.VMEM)] * 2,
        scratch_shapes=[
            pltpu.VMEM((rows, n * ka), left_factor.dtype),
            pltpu.VMEM((m * kb, cols), right_factor.dtype),
            pltpu.VMEM((n, chunks, 128), jnp.float32),
            pltpu.VMEM((n, 8, 128), jnp.float32),
            pltpu.VMEM((chunks, 128), jnp.float32),
            dma((2,)),
            dma((2, n, chunks)),
            dma((n, chunks)),
            dma((chips,)),
            dma((chips,)),
            dma((m,)),
            dma((2, n)),
            dma((2, n)),
        ],
        compiler_params=pltpu.CompilerParams(
            collective_id=0,
            has_side_effects=True,
            vmem_limit_bytes=VMEM_BYTES - rows * cols * 4 - 2**19,
        ),
    )(left_factor, right_factor)
    return pl.pallas_call(
        finish,
        out_shape=jax.ShapeDtypeStruct((rows, cols), jnp.float32),
        in_specs=[pl.BlockSpec(memory_space=pltpu.VMEM)] * 2,
        out_specs=pl.BlockSpec(memory_space=pl.ANY),
        scratch_shapes=[pltpu.VMEM((TAIL, CHUNK, cols), jnp.float32), dma((chunks,))],
        compiler_params=pltpu.CompilerParams(vmem_limit_bytes=TAIL * CHUNK * cols * 4 + 2 * 2**20),
    )(product, scale)


def solution(mesh):
    placed = (P("gy", "gx"), P("gy", "gx"))
    return jax.shard_map(
        functools.partial(per_device, mesh.shape["gy"], mesh.shape["gx"]),
        mesh=mesh,
        in_specs=placed,
        out_specs=P("gy", "gx"),
        check_vma=False,
    )
```
